32 devices in a mesh: tm: 4 (over x, core), space: 8 (over z, y).
Axes of the slice: x: 2, y: 2, z: 4, core: 2. Of those that a mesh axis runs over, the one named last changes fastest.
Arguments:
- span_opening: float32 [4, 32, 64, 128], P('tm', 'space'), may hold values from -8 to 8
- source_power: float32 [4, 2, 32, 64, 128], P('tm', None, 'space'), may hold values from -24 to 24
- warmth_retention: float32 [32, 64, 128], P('space'), may hold values from 0.02 to 0.4
Outputs:
- fpoint: float32 [4, 32, 64, 128], P('tm', 'space')
- updated: float32 [4, 32, 64, 128], P('tm', 'space')
The draws below stay inside these ranges and needn't reach their ends.
All inputs are finite; a program needn't handle non-finite values.
Results may differ from the reference program's by a relative error of at most 0.0001.
Values sent between devices are 32-bit elements; how exact they have to be, the bound alone decides.
A program may use at most 64 MiB of HBM per device.

```python
import math
import jax
import jax.numpy as jnp

NY = 64
NX = 128
STEPS = 2
COARSE_SWEEPS = 24
GROUPS = 4
NZ = 32


def draw_source_power(key, part):
    rough = 4.0 * jax.random.normal(key, (GROUPS, STEPS, NZ, NY, NX), jnp.float32)
    return jnp.clip(rough, -24.0, 24.0)


def shard_levels(rng, extent, pieces, smallest, largest):
    level, own = 1.0, jax.random.fold_in(rng, 6)
    for axis_at, blocks in pieces:
        steps = jnp.exp(jax.random.uniform(jax.random.fold_in(own, axis_at), (blocks,), jnp.float32, smallest / len(pieces), largest / len(pieces)))
        level = level * jnp.repeat(steps, extent[axis_at] // blocks).reshape([-1 if axis == axis_at else 1 for axis in range(len(extent))])
    return level


def scatter_about(own_key, shape, scale, reach, cuts=(), held_as=jnp.bfloat16):
    loudness = shard_levels(own_key, shape, cuts, -0.22, 0.18) if cuts else 1.0
    result = jax.random.normal(own_key, shape, jnp.float32) * scale * loudness
    return jnp.minimum(jnp.maximum(result, -reach), reach).astype(held_as)


def setup_inputs(seed: int = 0) -> dict:
    arg_keys = jax.random.split(jax.random.key(seed), 4)
    span_opening = scatter_about(arg_keys[0], (GROUPS, NZ, NY, NX), 2.0, 8.0, ((0, 4), (1, 8)), jnp.float32)
    source_power = draw_source_power(jax.random.fold_in(arg_keys[3], 71), 0)
    warmth_retention = jnp.clip(jnp.exp(math.log(0.4) - 2.9957323 * jax.random.uniform(arg_keys[2], (NZ, NY, NX), jnp.float32) ** shard_levels(arg_keys[2], (NZ, NY, NX), ((0, 8),), -0.2, 0.2)), 0.02, 0.4)
    return {"span_opening": span_opening, "source_power": source_power, "warmth_retention": warmth_retention}


relax_weight = 0.8


def mean_to_rougher(field):
    extent_layout = field.shape
    blocks = field.reshape(extent_layout[0] // 2, 2, extent_layout[1] // 2, 2, extent_layout[2] // 2, 2)
    return blocks.mean(axis=(1, 3, 5))


def lift_to_finer(field):
    extent_layout = field.shape
    grown = jnp.broadcast_to(field[:, None, :, None, :, None], (extent_layout[0], 2, extent_layout[1], 2, extent_layout[2], 2))
    return grown.reshape(2 * extent_layout[0], 2 * extent_layout[1], 2 * extent_layout[2])


def neighbour_sum(field, padded):
    flat = jnp.pad(field, ((0, 0), (1, 1), (1, 1)))
    total = padded[2:] + padded[:-2]
    total = total + flat[:, 2:, 1:-1] + flat[:, :-2, 1:-1]
    return total + flat[:, 1:-1, 2:] + flat[:, 1:-1, :-2]


def apply_nearby_part(field, retention_quantities, conductance):
    padded = jnp.pad(field, ((1, 1), (0, 0), (0, 0)))
    return (retention_quantities + 6.0 * conductance) * field - conductance * neighbour_sum(field, padded)


def bottom_grid_inversion(load_components, retention_quantities):
    conductance = 0.125
    diagonal = retention_quantities + 6.0 * conductance
    first_approximation = relax_weight * load_components / diagonal
    for sweep_index in range(COARSE_SWEEPS - 1):
        first_approximation = first_approximation + relax_weight * (load_components - apply_nearby_part(first_approximation, retention_quantities, conductance)) / diagonal
    return first_approximation


def personal_hierarchy_cycle(load_components, volume_holdings, hierarchy_layers):
    if hierarchy_layers == 3:
        return bottom_grid_inversion(load_components, volume_holdings[3])
    conductance = 0.5 ** hierarchy_layers
    retention_quantities = volume_holdings[hierarchy_layers]
    diagonal = retention_quantities + 6.0 * conductance
    first_approximation = relax_weight * load_components / diagonal
    first_approximation = first_approximation + relax_weight * (load_components - apply_nearby_part(first_approximation, retention_quantities, conductance)) / diagonal
    further_moments = load_components - apply_nearby_part(first_approximation, retention_quantities, conductance)
    first_approximation = first_approximation + lift_to_finer(personal_hierarchy_cycle(mean_to_rougher(further_moments), volume_holdings, hierarchy_layers + 1))
    for sweep_index in range(2):
        first_approximation = first_approximation + relax_weight * (load_components - apply_nearby_part(first_approximation, retention_quantities, conductance)) / diagonal
    return first_approximation


def reference(span_opening, source_power, warmth_retention):
    volume_holdings = [warmth_retention]
    for level_index in range(3):
        volume_holdings.append(mean_to_rougher(volume_holdings[-1]))
    fpoints = []
    closing_results = []
    for moment_packet in range(GROUPS):
        warmth_distribution = span_opening[moment_packet]
        opening_condition = warmth_distribution
        for moment_count in range(STEPS):
            warmth_distribution = personal_hierarchy_cycle(warmth_retention * warmth_distribution + source_power[moment_packet, moment_count], volume_holdings, 0)
            if moment_count == 0:
                opening_condition = warmth_distribution
        fpoints.append(opening_condition)
        closing_results.append(warmth_distribution)
    updated = jnp.stack([span_opening[0]] + closing_results[:-1])
    return jnp.stack(fpoints), updated
```

```python
import functools

import jax
import jax.numpy as jnp
from jax import lax
from jax.experimental import pallas as pl
from jax.experimental.pallas import tpu as pltpu
from jax.sharding import PartitionSpec as P

COARSE_SWEEPS = 24
W = 0.8
F32 = jnp.float32
MESH = pl.DeviceIdType.MESH


def iota(shape, dim):
    return lax.broadcasted_iota(jnp.int32, shape, dim)


def dot(a, b):
    return jnp.dot(a, b, precision=lax.Precision.HIGHEST, preferred_element_type=F32)


def picks(lanes, pick, scale):
    src, dst = iota((lanes, lanes), 0), iota((lanes, lanes), 1)
    return jnp.where(pick(src, dst), scale, 0.0).astype(F32)


def in_plane(x, width):
    rows, lanes = x.shape[1], x.shape[2]
    lane, row = iota(x.shape, 2), iota(x.shape, 1)
    left, right = pltpu.roll(x, 1, 2), pltpu.roll(x, lanes - 1, 2)
    if width > lanes // 4:
        left = jnp.where(lane % width == 0, 0.0, left)
        right = jnp.where(lane % width == width - 1, 0.0, right)
    up = jnp.where(row == 0, 0.0, pltpu.roll(x, 1, 1))
    down = jnp.where(row == rows - 1, 0.0, pltpu.roll(x, rows - 1, 1))
    return (left + right) + (up + down)


def shifted(x):
    zero = jnp.zeros((1,) + x.shape[1:], F32)
    return jnp.concatenate([zero, x[:-1]], 0), jnp.concatenate([x[1:], zero], 0)


def sum_planes(x, width):
    before, after = shifted(x)
    return in_plane(x, width) + (before + after)


def sum_packed(x, width):
    half = pltpu.roll(x, width, 2)
    before, after = shifted(half)
    return in_plane(x, width) + (half + jnp.where(iota(x.shape, 2) < width, before, after))


def sum_inner(x, width):
    return in_plane(x[1:-1], width) + (x[:-2] + x[2:])


def flat(x):
    return x.reshape(x.shape[0] * x.shape[1], x.shape[2])


def kernel(
    parts, spans, steps,
    open_ref, src_ref, cap_in,
    fp_ref, up_ref,
    u0, src, cap, cx, gcap, gr, own, x1p, tmp, fin,
    in_sem, hs, hr, ks, kr, gs, gv, ts,
):
    me, span = lax.axis_index("space"), lax.axis_index("tm")
    depth, rows, lanes = open_ref.shape
    half = lanes // 2

    barrier = pltpu.get_barrier_semaphore()
    for k in range(1, parts):
        pl.semaphore_signal(barrier, inc=1, device_id={"space": (me + k) % parts}, device_id_type=MESH)
    for k in (1, spans - 1):
        pl.semaphore_signal(barrier, inc=1, device_id={"tm": (span + k) % spans}, device_id_type=MESH)

    loads = [
        pltpu.make_async_copy(cap_in, cap.at[pl.ds(2, depth)], in_sem.at[0]),
        pltpu.make_async_copy(open_ref, u0, in_sem.at[1]),
        pltpu.make_async_copy(src_ref, src, in_sem.at[2]),
    ]
    for load in loads:
        load.start()

    down_lo = picks(lanes, lambda s, d: (s // 2 == d) & (d < half), 0.125)
    down_hi = picks(lanes, lambda s, d: s // 2 + half == d, 0.125)
    down_2 = picks(lanes, lambda s, d: (s % half) // 2 == d, 0.125)
    down_3 = picks(lanes, lambda s, d: (s // 2 == d) & (s < half // 2), 0.125)
    up_lo = picks(lanes, lambda s, d: d // 2 == s, 1.0)
    up_hi = picks(lanes, lambda s, d: d // 2 + half == s, 1.0)
    up_2 = picks(lanes, lambda s, d: (d % half) // 2 == s, 1.0)
    up_3 = picks(lanes, lambda s, d: (d // 2 == s) & (d < half // 2), 1.0)

    def pair_rows(x):
        n, r, w = x.shape
        tmp[pl.ds(0, n * r), :] = flat(x)
        return tmp[pl.ds(0, n * r // 2, 2), :] + tmp[pl.ds(1, n * r // 2, 2), :]

    def twice_rows(x, planes):
        r = x.shape[0]
        tmp[pl.ds(0, r, 2), :] = x
        tmp[pl.ds(1, r, 2), :] = x
        return tmp[pl.ds(0, 2 * r), :].reshape(planes, 2 * r // planes, lanes)

    def pack(x):
        s = pair_rows(x.reshape(depth // 2, 2, rows, lanes).sum(1))
        n = rows // 2
        return dot(s[:n], down_lo) + dot(s[n:], down_hi)

    def to_2(x):
        return dot(pair_rows(x), down_2).reshape(parts, rows // 4, lanes)

    def to_3(x):
        s = x.reshape(parts // 2, 2, rows // 4, lanes).sum(1)
        return dot(pair_rows(s), down_3).reshape(parts // 2, rows // 8, lanes)

    def halo(buf, sends, recvs, at, up, down):
        to_next = pltpu.make_async_remote_copy(
            buf.at[pl.ds(*up[0])], buf.at[pl.ds(*up[1])], sends.at[at], recvs.at[at],
            device_id={"space": (me + 1) % parts}, device_id_type=MESH)
        to_prev = pltpu.make_async_remote_copy(
            buf.at[pl.ds(*down[0])], buf.at[pl.ds(*down[1])], sends.at[at + 1], recvs.at[at + 1],
            device_id={"space": (me + parts - 1) % parts}, device_id_type=MESH)
        return to_next, to_prev

    def begin(pair):
        @pl.when(me < parts - 1)
        def _():
            pair[0].start()

        @pl.when(me > 0)
        def _():
            pair[1].start()

    def arrive(pair):
        @pl.when(me > 0)
        def _():
            pair[0].wait_recv()

        @pl.when(me < parts - 1)
        def _():
            pair[1].wait_recv()

    def sent(pair):
        @pl.when(me < parts - 1)
        def _():
            pair[0].wait_send()

        @pl.when(me > 0)
        def _():
            pair[1].wait_send()

    def gather(buf, sends, recvs, row):
        return [
            pltpu.make_async_remote_copy(
                buf.at[me], buf.at[me], sends.at[row, k], recvs.at[row, k],
                device_id={"space": (me + k) % parts}, device_id_type=MESH)
            for k in range(1, parts)
        ]

    near = [halo(cx.at[t], hs, hr, 4 * t, ((depth + 1, 2), (1, 2)), ((3, 2), (depth + 3, 2))) for t in range(steps)]
    far = [halo(cx.at[t], hs, hr, 4 * t + 2, ((depth, 1), (0, 1)), ((5, 1), (depth + 5, 1))) for t in range(steps)]
    caps = halo(cap, ks, kr, 0, ((depth, 2), (0, 2)), ((2, 2), (depth + 2, 2)))
    gather_cap = gather(gcap, gs, gv, 0)
    gather_r = [gather(gr.at[t], gs, gv, 1 + t) for t in range(steps)]

    @pl.when(me == 0)
    def _():
        cap[0:2] = jnp.zeros((2, rows, lanes), F32)
        for t in range(steps):
            cx[t, 0:3] = jnp.zeros((3, rows, lanes), F32)

    @pl.when(me == parts - 1)
    def _():
        cap[depth + 2:] = jnp.zeros((2, rows, lanes), F32)
        for t in range(steps):
            cx[t, depth + 3:] = jnp.zeros((3, rows, lanes), F32)

    x1p[0] = jnp.zeros(x1p.shape[1:], F32)
    x1p[parts + 1] = jnp.zeros(x1p.shape[1:], F32)

    loads[0].wait()
    mine = cap[2:2 + depth]
    gcap[me] = pack(mine)
    loads[1].wait()
    loads[2].wait()
    b = mine * u0[...] + src[0]
    own[...] = b
    cx[0, 3:3 + depth] = b * (W / (mine + 6.0))

    pl.semaphore_wait(barrier, parts - 1 + 2)
    begin(near[0])
    begin(caps)
    for copy in gather_cap:
        copy.start()
    begin(far[0])

    arrive(caps)
    plane = me * depth - 2 + iota((depth + 4, 1, 1), 0)
    inside = (plane >= 0) & (plane < parts * depth)
    a0 = jnp.where(inside, W / (cap[...] + 6.0), 0.0)
    cells = None

    for t in range(steps):
        last = t == steps - 1
        arrive(near[t])
        c = cx[t, 1:depth + 5]
        x = 1.2 * c[1:-1] + a0[1:-1] * sum_inner(c, lanes)
        inner = x[1:-1]
        d0 = cap[2:2 + depth] + 6.0
        r = own[...] - d0 * inner + sum_inner(x, lanes)
        gr[t, me] = pack(r)
        for copy in gather_r[t]:
            copy.start()

        arrive(far[t])
        first = 1.2 * cx[t, 1:2] + a0[0:1] * sum_inner(cx[t, 0:3], lanes)
        final = 1.2 * cx[t, depth + 4:depth + 5] + a0[-1:] * sum_inner(cx[t, depth + 3:depth + 6], lanes)
        x = jnp.concatenate([first, x, final], 0)

        if t == 0:
            for copy in gather_cap:
                copy.wait_recv()
            cap1 = gcap[...]
            i1 = W / (cap1 + 3.0)
            cap2 = to_2(cap1)
            i2 = jnp.where(iota(cap2.shape, 2) < lanes // 4, W / (cap2 + 1.5), 0.0)
            cap3 = to_3(cap2)
            i3 = jnp.where(iota(cap3.shape, 2) < lanes // 8, W / (cap3 + 0.75), 0.0)
            a1, a2, a3 = 0.5 * i1, 0.25 * i2, 0.125 * i3

        for copy in gather_r[t]:
            copy.wait_recv()
        b1 = gr[t]
        c1 = b1 * i1
        y1 = 1.2 * c1 + a1 * sum_packed(c1, half)
        r1 = b1 - (cap1 + 3.0) * y1 + 0.5 * sum_packed(y1, half)
        b2 = to_2(r1)
        c2 = b2 * i2
        y2 = 1.2 * c2 + a2 * sum_planes(c2, lanes // 4)
        r2 = b2 - (cap2 + 1.5) * y2 + 0.25 * sum_planes(y2, lanes // 4)
        c3 = to_3(r2) * i3
        y3 = lax.fori_loop(
            0, COARSE_SWEEPS - 1,
            lambda _, y: (0.2 * y + c3) + a3 * sum_planes(y, lanes // 8), c3, unroll=True)
        lift = twice_rows(dot(flat(y3), up_3), parts // 2)
        lift = jnp.broadcast_to(lift[:, None], (parts // 2, 2) + lift.shape[1:]).reshape(y2.shape)
        y2 = y2 + lift
        for _ in range(2):
            y2 = (0.2 * y2 + c2) + a2 * sum_planes(y2, lanes // 4)
        y1 = y1 + twice_rows(dot(flat(y2), up_2), parts)
        for _ in range(2):
            y1 = (0.2 * y1 + c1) + a1 * sum_packed(y1, half)
        x1p[1:parts + 1] = y1

        odd = dot(flat(x1p[pl.ds(me, 2)]), up_hi)
        even = dot(flat(x1p[pl.ds(me + 1, 2)]), up_lo)
        n = rows // 2
        lift = twice_rows(jnp.concatenate([odd[:n], even[:n], odd[n:], even[n:]], 0), depth // 2 + 2)
        lift = jnp.broadcast_to(lift[:, None], (depth // 2 + 2, 2) + lift.shape[1:]).reshape(x.shape)
        x = x + lift
        x = (0.2 * x[1:-1] + cx[t, 2:depth + 4]) + a0[1:-1] * sum_inner(x, lanes)
        x = (0.2 * x[1:-1] + cx[t, 3:depth + 3]) + a0[2:-2] * sum_inner(x, lanes)
        if t == 0:
            fp_ref[...] = x
        if not last:
            b = cap[2:2 + depth] * x + src[t + 1]
            own[...] = b
            cx[t + 1, 3:3 + depth] = b * a0[2:-2]
            begin(near[t + 1])
            begin(far[t + 1])
        else:
            fin[...] = x

    onward = pltpu.make_async_remote_copy(
        fin, up_ref, ts.at[0], ts.at[1],
        device_id={"tm": (span + 1) % spans}, device_id_type=MESH)

    @pl.when(span < spans - 1)
    def _():
        onward.start()

    @pl.when(span == 0)
    def _():
        up_ref[...] = u0[...]

    for pair in near + far + [caps]:
        sent(pair)
    for copies in [gather_cap] + gather_r:
        for copy in copies:
            copy.wait_send()

    @pl.when(span < spans - 1)
    def _():
        onward.wait_send()

    @pl.when(span > 0)
    def _():
        onward.wait_recv()


def shards(span_opening, source_power, warmth_retention):
    parts, spans = lax.axis_size("space"), lax.axis_size("tm")
    steps = source_power.shape[1]
    depth, rows, lanes = warmth_retention.shape
    slab = jax.ShapeDtypeStruct((depth, rows, lanes), F32)
    vmem = pl.BlockSpec(memory_space=pltpu.VMEM)
    dma = pltpu.SemaphoreType.DMA
    fpoint, updated = pl.pallas_call(
        functools.partial(kernel, parts, spans, steps),
        out_shape=(slab, slab),
        in_specs=[pl.BlockSpec(memory_space=pl.ANY)] * 3,
        out_specs=(vmem, vmem),
        scratch_shapes=[
            pltpu.VMEM((depth, rows, lanes), F32),
            pltpu.VMEM((steps, depth, rows, lanes), F32),
            pltpu.VMEM((depth + 4, rows, lanes), F32),
            pltpu.VMEM((steps, depth + 6, rows, lanes), F32),
            pltpu.VMEM((parts, rows // 2, lanes), F32),
            pltpu.VMEM((steps, parts, rows // 2, lanes), F32),
            pltpu.VMEM((depth, rows, lanes), F32),
            pltpu.VMEM((parts + 2, rows // 2, lanes), F32),
            pltpu.VMEM((max(parts * rows // 2, (depth // 2 + 2) * rows), lanes), F32),
            pltpu.VMEM((depth, rows, lanes), F32),
            dma((3,)), dma((4 * steps,)), dma((4 * steps,)), dma((2,)), dma((2,)),
            dma((1 + steps, parts)), dma((1 + steps, parts)), dma((2,)),
        ],
        compiler_params=pltpu.CompilerParams(
            collective_id=0, has_side_effects=True, vmem_limit_bytes=48 * 1024 * 1024
        ),
    )(span_opening[0], source_power[0], warmth_retention)
    return fpoint[None], updated[None]


def solution(mesh):
    in_specs = (
        P("tm", "space", None, None),
        P("tm", None, "space", None, None),
        P("space", None, None),
    )
    out_specs = (P("tm", "space", None, None), P("tm", "space", None, None))
    return jax.shard_map(shards, mesh=mesh, in_specs=in_specs, out_specs=out_specs, check_vma=False)
```

```python
import functools

import jax
import jax.numpy as jnp
from jax import lax
from jax.experimental import pallas as pl
from jax.experimental.pallas import tpu as pltpu
from jax.sharding import PartitionSpec as P

COARSE_SWEEPS = 24
W = 0.8
F32 = jnp.float32
MESH = pl.DeviceIdType.MESH


def iota(shape, dim):
    return lax.broadcasted_iota(jnp.int32, shape, dim)


def dot(a, b):
    return jnp.dot(a, b, precision=lax.Precision.HIGHEST, preferred_element_type=F32)


def picks(lanes, pick, scale):
    src, dst = iota((lanes, lanes), 0), iota((lanes, lanes), 1)
    return jnp.where(pick(src, dst), scale, 0.0).astype(F32)


def in_plane(x, width):
    rows, lanes = x.shape[1], x.shape[2]
    lane, row = iota(x.shape, 2), iota(x.shape, 1)
    left, right = pltpu.roll(x, 1, 2), pltpu.roll(x, lanes - 1, 2)
    if width > lanes // 4:
        left = jnp.where(lane % width == 0, 0.0, left)
        right = jnp.where(lane % width == width - 1, 0.0, right)
    up = jnp.where(row == 0, 0.0, pltpu.roll(x, 1, 1))
    down = jnp.where(row == rows - 1, 0.0, pltpu.roll(x, rows - 1, 1))
    return (left + right) + (up + down)


def shifted(x):
    zero = jnp.zeros((1,) + x.shape[1:], F32)
    return jnp.concatenate([zero, x[:-1]], 0), jnp.concatenate([x[1:], zero], 0)


def sum_planes(x, width):
    before, after = shifted(x)
    return in_plane(x, width) + (before + after)


def sum_packed(x, width):
    half = pltpu.roll(x, width, 2)
    before, after = shifted(half)
    return in_plane(x, width) + (half + jnp.where(iota(x.shape, 2) < width, before, after))


def sum_inner(x, width):
    return in_plane(x[1:-1], width) + (x[:-2] + x[2:])


def flat(x):
    return x.reshape(x.shape[0] * x.shape[1], x.shape[2])


def kernel(
    parts, spans, steps,
    open_ref, src_ref, cap_in,
    fp_ref, up_ref,
    u0, src, cap, cx, gcap, gr, own, x1p, tmp, fin,
    in_sem, hs, hr, ks, kr, gs, gv, ts,
):
    me, span = lax.axis_index("space"), lax.axis_index("tm")
    depth, rows, lanes = open_ref.shape
    half = lanes // 2

    barrier = pltpu.get_barrier_semaphore()
    for k in range(1, parts):
        pl.semaphore_signal(barrier, inc=1, device_id={"space": (me + k) % parts}, device_id_type=MESH)
    for k in (1, spans - 1):
        pl.semaphore_signal(barrier, inc=1, device_id={"tm": (span + k) % spans}, device_id_type=MESH)

    loads = [
        pltpu.make_async_copy(cap_in, cap.at[pl.ds(2, depth)], in_sem.at[0]),
        pltpu.make_async_copy(open_ref, u0, in_sem.at[1]),
        pltpu.make_async_copy(src_ref, src, in_sem.at[2]),
    ]
    for load in loads:
        load.start()

    down_lo = picks(lanes, lambda s, d: (s // 2 == d) & (d < half), 0.125)
    down_hi = picks(lanes, lambda s, d: s // 2 + half == d, 0.125)
    down_2 = picks(lanes, lambda s, d: (s % half) // 2 == d, 0.125)
    down_3 = picks(lanes, lambda s, d: (s // 2 == d) & (s < half // 2), 0.125)
    up_lo = picks(lanes, lambda s, d: d // 2 == s, 1.0)
    up_hi = picks(lanes, lambda s, d: d // 2 + half == s, 1.0)
    up_2 = picks(lanes, lambda s, d: (d % half) // 2 == s, 1.0)
    up_3 = picks(lanes, lambda s, d: (d // 2 == s) & (d < half // 2), 1.0)

    def pair_rows(x):
        n, r, w = x.shape
        tmp[pl.ds(0, n * r), :] = flat(x)
        return tmp[pl.ds(0, n * r // 2, 2), :] + tmp[pl.ds(1, n * r // 2, 2), :]

    def twice_rows(x, planes):
        r = x.shape[0]
        tmp[pl.ds(0, r, 2), :] = x
        tmp[pl.ds(1, r, 2), :] = x
        return tmp[pl.ds(0, 2 * r), :].reshape(planes, 2 * r // planes, lanes)

    def pack(x):
        s = pair_rows(x.reshape(depth // 2, 2, rows, lanes).sum(1))
        n = rows // 2
        return dot(s[:n], down_lo) + dot(s[n:], down_hi)

    def to_2(x):
        return dot(pair_rows(x), down_2).reshape(parts, rows // 4, lanes)

    def to_3(x):
        s = x.reshape(parts // 2, 2, rows // 4, lanes).sum(1)
        return dot(pair_rows(s), down_3).reshape(parts // 2, rows // 8, lanes)

    def halo(buf, sends, recvs, at, up, down):
        to_next = pltpu.make_async_remote_copy(
            buf.at[pl.ds(*up[0])], buf.at[pl.ds(*up[1])], sends.at[at], recvs.at[at],
            device_id={"space": (me + 1) % parts}, device_id_type=MESH)
        to_prev = pltpu.make_async_remote_copy(
            buf.at[pl.ds(*down[0])], buf.at[pl.ds(*down[1])], sends.at[at + 1], recvs.at[at + 1],
            device_id={"space": (me + parts - 1) % parts}, device_id_type=MESH)
        return to_next, to_prev

    def begin(pair):
        @pl.when(me < parts - 1)
        def _():
            pair[0].start()

        @pl.when(me > 0)
        def _():
            pair[1].start()

    def arrive(pair):
        @pl.when(me > 0)
        def _():
            pair[0].wait_recv()

        @pl.when(me < parts - 1)
        def _():
            pair[1].wait_recv()

    def sent(pair):
        @pl.when(me < parts - 1)
        def _():
            pair[0].wait_send()

        @pl.when(me > 0)
        def _():
            pair[1].wait_send()

    def gather(buf, sends, recvs, row):
        return [
            pltpu.make_async_remote_copy(
                buf.at[me], buf.at[me], sends.at[row, k], recvs.at[row, k],
                device_id={"space": (me + k) % parts}, device_id_type=MESH)
            for k in range(1, parts)
        ]

    near = [halo(cx.at[t], hs, hr, 4 * t, ((depth + 1, 2), (1, 2)), ((3, 2), (depth + 3, 2))) for t in range(steps)]
    far = [halo(cx.at[t], hs, hr, 4 * t + 2, ((depth, 1), (0, 1)), ((5, 1), (depth + 5, 1))) for t in range(steps)]
    cap_near = halo(cap, ks, kr, 0, ((depth + 1, 1), (1, 1)), ((2, 1), (depth + 2, 1)))
    cap_far = halo(cap, ks, kr, 2, ((depth, 1), (0, 1)), ((3, 1), (depth + 3, 1)))
    gather_cap = gather(gcap, gs, gv, 0)
    gather_r = [gather(gr.at[t], gs, gv, 1 + t) for t in range(steps)]

    @pl.when(me == 0)
    def _():
        cap[0:2] = jnp.zeros((2, rows, lanes), F32)
        for t in range(steps):
            cx[t, 0:3] = jnp.zeros((3, rows, lanes), F32)

    @pl.when(me == parts - 1)
    def _():
        cap[depth + 2:] = jnp.zeros((2, rows, lanes), F32)
        for t in range(steps):
            cx[t, depth + 3:] = jnp.zeros((3, rows, lanes), F32)

    x1p[0] = jnp.zeros(x1p.shape[1:], F32)
    x1p[parts + 1] = jnp.zeros(x1p.shape[1:], F32)

    loads[0].wait()
    mine = cap[2:2 + depth]
    gcap[me] = pack(mine)
    loads[1].wait()
    loads[2].wait()
    b = mine * u0[...] + src[0]
    own[...] = b
    cx[0, 3:3 + depth] = b * (W / (mine + 6.0))

    pl.semaphore_wait(barrier, parts - 1 + 2)
    begin(cap_near)
    begin(near[0])
    for copy in gather_cap:
        copy.start()

    def weights(start, count):
        plane = me * depth - 2 + start + iota((count, 1, 1), 0)
        inside = (plane >= 0) & (plane < parts * depth)
        return jnp.where(inside, W / (cap[start:start + count] + 6.0), 0.0)

    arrive(cap_near)
    a = weights(1, depth + 2)

    for t in range(steps):
        last = t == steps - 1
        arrive(near[t])
        c = cx[t, 1:depth + 5]
        x = 1.2 * c[1:-1] + a * sum_inner(c, lanes)
        inner = x[1:-1]
        d0 = cap[2:2 + depth] + 6.0
        r = own[...] - d0 * inner + sum_inner(x, lanes)
        gr[t, me] = pack(r)
        for copy in gather_r[t]:
            copy.start()
        begin(far[t])
        if t == 0:
            begin(cap_far)
            for copy in gather_cap:
                copy.wait_recv()
            cap1 = gcap[...]
            i1 = W / (cap1 + 3.0)
            cap2 = to_2(cap1)
            i2 = jnp.where(iota(cap2.shape, 2) < lanes // 4, W / (cap2 + 1.5), 0.0)
            cap3 = to_3(cap2)
            i3 = jnp.where(iota(cap3.shape, 2) < lanes // 8, W / (cap3 + 0.75), 0.0)
            a1, a2, a3 = 0.5 * i1, 0.25 * i2, 0.125 * i3

        for copy in gather_r[t]:
            copy.wait_recv()
        b1 = gr[t]
        c1 = b1 * i1
        y1 = 1.2 * c1 + a1 * sum_packed(c1, half)
        r1 = b1 - (cap1 + 3.0) * y1 + 0.5 * sum_packed(y1, half)
        b2 = to_2(r1)
        c2 = b2 * i2
        y2 = 1.2 * c2 + a2 * sum_planes(c2, lanes // 4)
        r2 = b2 - (cap2 + 1.5) * y2 + 0.25 * sum_planes(y2, lanes // 4)
        c3 = to_3(r2) * i3
        y3 = lax.fori_loop(
            0, COARSE_SWEEPS - 1,
            lambda _, y: (0.2 * y + c3) + a3 * sum_planes(y, lanes // 8), c3, unroll=True)
        lift = twice_rows(dot(flat(y3), up_3), parts // 2)
        lift = jnp.broadcast_to(lift[:, None], (parts // 2, 2) + lift.shape[1:]).reshape(y2.shape)
        y2 = y2 + lift
        for _ in range(2):
            y2 = (0.2 * y2 + c2) + a2 * sum_planes(y2, lanes // 4)
        y1 = y1 + twice_rows(dot(flat(y2), up_2), parts)
        for _ in range(2):
            y1 = (0.2 * y1 + c1) + a1 * sum_packed(y1, half)
        x1p[1:parts + 1] = y1

        odd = dot(flat(x1p[pl.ds(me, 2)]), up_hi)
        even = dot(flat(x1p[pl.ds(me + 1, 2)]), up_lo)
        n = rows // 2
        lift = twice_rows(jnp.concatenate([odd[:n], even[:n], odd[n:], even[n:]], 0), depth // 2 + 2)
        lift = jnp.broadcast_to(lift[:, None], (depth // 2 + 2, 2) + lift.shape[1:]).reshape(depth + 4, rows, lanes)
        arrive(far[t])
        if t == 0:
            arrive(cap_far)
            a_lo, a_hi = weights(0, 1), weights(depth + 3, 1)
        first = 1.2 * cx[t, 1:2] + a_lo * sum_inner(cx[t, 0:3], lanes)
        final = 1.2 * cx[t, depth + 4:depth + 5] + a_hi * sum_inner(cx[t, depth + 3:depth + 6], lanes)
        x = jnp.concatenate([first, x, final], 0) + lift
        x = (0.2 * x[1:-1] + cx[t, 2:depth + 4]) + a * sum_inner(x, lanes)
        x = (0.2 * x[1:-1] + cx[t, 3:depth + 3]) + a[1:-1] * sum_inner(x, lanes)
        if t == 0:
            fp_ref[...] = x
        if not last:
            b = cap[2:2 + depth] * x + src[t + 1]
            own[...] = b
            cx[t + 1, 3:3 + depth] = b * a[1:-1]
            begin(near[t + 1])
        else:
            fin[...] = x

    onward = pltpu.make_async_remote_copy(
        fin, up_ref, ts.at[0], ts.at[1],
        device_id={"tm": (span + 1) % spans}, device_id_type=MESH)

    @pl.when(span < spans - 1)
    def _():
        onward.start()

    @pl.when(span == 0)
    def _():
        up_ref[...] = u0[...]

    for pair in near + far + [cap_near, cap_far]:
        sent(pair)
    for copies in [gather_cap] + gather_r:
        for copy in copies:
            copy.wait_send()

    @pl.when(span < spans - 1)
    def _():
        onward.wait_send()

    @pl.when(span > 0)
    def _():
        onward.wait_recv()


def shards(span_opening, source_power, warmth_retention):
    parts, spans = lax.axis_size("space"), lax.axis_size("tm")
    steps = source_power.shape[1]
    depth, rows, lanes = warmth_retention.shape
    slab = jax.ShapeDtypeStruct((depth, rows, lanes), F32)
    vmem = pl.BlockSpec(memory_space=pltpu.VMEM)
    dma = pltpu.SemaphoreType.DMA
    fpoint, updated = pl.pallas_call(
        functools.partial(kernel, parts, spans, steps),
        out_shape=(pltpu.VMEM(slab.shape, F32),) * 2,
        in_specs=[pl.BlockSpec(memory_space=pl.ANY)] * 3,
        out_specs=(vmem, vmem),
        scratch_shapes=[
            pltpu.VMEM((depth, rows, lanes), F32),
            pltpu.VMEM((steps, depth, rows, lanes), F32),
            pltpu.VMEM((depth + 4, rows, lanes), F32),
            pltpu.VMEM((steps, depth + 6, rows, lanes), F32),
            pltpu.VMEM((parts, rows // 2, lanes), F32),
            pltpu.VMEM((steps, parts, rows // 2, lanes), F32),
            pltpu.VMEM((depth, rows, lanes), F32),
            pltpu.VMEM((parts + 2, rows // 2, lanes), F32),
            pltpu.VMEM((max(parts * rows // 2, (depth // 2 + 2) * rows), lanes), F32),
            pltpu.VMEM((depth, rows, lanes), F32),
            dma((3,)), dma((4 * steps,)), dma((4 * steps,)), dma((4,)), dma((4,)),
            dma((1 + steps, parts)), dma((1 + steps, parts)), dma((2,)),
        ],
        compiler_params=pltpu.CompilerParams(
            collective_id=0, has_side_effects=True, vmem_limit_bytes=67043328 - 2 * 4 * slab.size
        ),
    )(span_opening[0], source_power[0], warmth_retention)
    return fpoint[None], updated[None]


def solution(mesh):
    in_specs = (
        P("tm", "space", None, None),
        P("tm", None, "space", None, None),
        P("space", None, None),
    )
    out_specs = (P("tm", "space", None, None), P("tm", "space", None, None))
    return jax.shard_map(shards, mesh=mesh, in_specs=in_specs, out_specs=out_specs, check_vma=False)
```

```python
import functools

import jax
import jax.numpy as jnp
from jax import lax
from jax.experimental import pallas as pl
from jax.experimental.pallas import tpu as pltpu
from jax.sharding import PartitionSpec as P

COARSE_SWEEPS = 24
W = 0.8
F32 = jnp.float32
MESH = pl.DeviceIdType.MESH


def iota(shape, dim):
    return lax.broadcasted_iota(jnp.int32, shape, dim)


def dot(a, b):
    return jnp.dot(a, b, precision=lax.Precision.HIGHEST, preferred_element_type=F32)


def picks(lanes, pick, scale):
    src, dst = iota((lanes, lanes), 0), iota((lanes, lanes), 1)
    return jnp.where(pick(src, dst), scale, 0.0).astype(F32)


def in_plane(x, width):
    rows, lanes = x.shape[1], x.shape[2]
    lane, row = iota(x.shape, 2), iota(x.shape, 1)
    left, right = pltpu.roll(x, 1, 2), pltpu.roll(x, lanes - 1, 2)
    if width > lanes // 4:
        left = jnp.where(lane % width == 0, 0.0, left)
        right = jnp.where(lane % width == width - 1, 0.0, right)
    up = jnp.where(row == 0, 0.0, pltpu.roll(x, 1, 1))
    down = jnp.where(row == rows - 1, 0.0, pltpu.roll(x, rows - 1, 1))
    return (left + right) + (up + down)


def shifted(x):
    zero = jnp.zeros((1,) + x.shape[1:], F32)
    return jnp.concatenate([zero, x[:-1]], 0), jnp.concatenate([x[1:], zero], 0)


def sum_planes(x, width):
    before, after = shifted(x)
    return in_plane(x, width) + (before + after)


def sum_packed(x, width):
    half = pltpu.roll(x, width, 2)
    before, after = shifted(half)
    return in_plane(x, width) + (half + jnp.where(iota(x.shape, 2) < width, before, after))


def sum_inner(x, width):
    return in_plane(x[1:-1], width) + (x[:-2] + x[2:])


def flat(x):
    return x.reshape(x.shape[0] * x.shape[1], x.shape[2])


def kernel(
    parts, spans, steps,
    open_ref, src_ref, cap_in,
    fp_ref, up_ref,
    u0, src0, src1, cap, c0, c1x, gcap, gr, own, x1p, tmp, fin,
    in_sem, hs, hr, ks, kr, fs, fr, gs, gv, ts,
):
    me, span = lax.axis_index("space"), lax.axis_index("tm")
    depth, rows, lanes = open_ref.shape
    half = lanes // 2

    barrier = pltpu.get_barrier_semaphore()
    for k in range(1, parts):
        pl.semaphore_signal(barrier, inc=1, device_id={"space": (me + k) % parts}, device_id_type=MESH)
    for k in range(1, spans):
        pl.semaphore_signal(barrier, inc=1, device_id={"tm": (span + k) % spans}, device_id_type=MESH)

    loads = [
        pltpu.make_async_copy(cap_in, cap.at[pl.ds(depth, depth)], in_sem.at[0]),
        pltpu.make_async_copy(open_ref, u0, in_sem.at[1]),
        pltpu.make_async_copy(src_ref.at[0], src0, in_sem.at[2]),
        pltpu.make_async_copy(src_ref.at[1], src1.at[pl.ds(2, depth)], in_sem.at[3]),
    ]
    for load in loads:
        load.start()

    down_lo = picks(lanes, lambda s, d: (s // 2 == d) & (d < half), 0.125)
    down_hi = picks(lanes, lambda s, d: s // 2 + half == d, 0.125)
    down_2 = picks(lanes, lambda s, d: (s % half) // 2 == d, 0.125)
    down_3 = picks(lanes, lambda s, d: (s // 2 == d) & (s < half // 2), 0.125)
    up_lo = picks(lanes, lambda s, d: d // 2 == s, 1.0)
    up_hi = picks(lanes, lambda s, d: d // 2 + half == s, 1.0)
    up_2 = picks(lanes, lambda s, d: (d % half) // 2 == s, 1.0)
    up_3 = picks(lanes, lambda s, d: (d // 2 == s) & (d < half // 2), 1.0)

    def pair_rows(x):
        n, r, w = x.shape
        tmp[pl.ds(0, n * r), :] = flat(x)
        return tmp[pl.ds(0, n * r // 2, 2), :] + tmp[pl.ds(1, n * r // 2, 2), :]

    def twice_rows(x, planes):
        r = x.shape[0]
        tmp[pl.ds(0, r, 2), :] = x
        tmp[pl.ds(1, r, 2), :] = x
        return tmp[pl.ds(0, 2 * r), :].reshape(planes, 2 * r // planes, lanes)

    def pack(x):
        s = pair_rows(x.reshape(depth // 2, 2, rows, lanes).sum(1))
        n = rows // 2
        return dot(s[:n], down_lo) + dot(s[n:], down_hi)

    def to_2(x):
        return dot(pair_rows(x), down_2).reshape(parts, rows // 4, lanes)

    def to_3(x):
        s = x.reshape(parts // 2, 2, rows // 4, lanes).sum(1)
        return dot(pair_rows(s), down_3).reshape(parts // 2, rows // 8, lanes)

    def halo(buf, sends, recvs, at, count, up, down, reach=1, rows_at=None):
        def cut(start):
            return buf.at[pl.ds(start, count)] if rows_at is None else buf.at[pl.ds(start, count), rows_at]

        ways = ((up, reach, at), (down, parts - reach, at + 1))
        pair = [
            pltpu.make_async_remote_copy(
                cut(way[0]), cut(way[1]), sends.at[sem], recvs.at[sem],
                device_id={"space": (me + by) % parts}, device_id_type=MESH)
            for way, by, sem in ways
        ]
        return pair + [reach]

    def begin(pair):
        @pl.when(me < parts - pair[2])
        def _():
            pair[0].start()

        @pl.when(me >= pair[2])
        def _():
            pair[1].start()

    def arrive(pair):
        @pl.when(me >= pair[2])
        def _():
            pair[0].wait_recv()

        @pl.when(me < parts - pair[2])
        def _():
            pair[1].wait_recv()

    def sent(pair):
        @pl.when(me < parts - pair[2])
        def _():
            pair[0].wait_send()

        @pl.when(me >= pair[2])
        def _():
            pair[1].wait_send()

    share = rows // spans
    my_rows = pl.ds(pl.multiple_of(span * share, share), share)

    def hand_on(at, count, below, above):
        def copies(start, sem):
            return [
                pltpu.make_async_remote_copy(
                    cap.at[pl.ds(start, count), my_rows], cap.at[pl.ds(start, count), my_rows],
                    fs.at[sem, k], fr.at[sem, k],
                    device_id={"tm": (span + k) % spans}, device_id_type=MESH)
                for k in range(1, spans)
            ]

        return copies(below, at), copies(above, at + 1)

    def each(pair, act):
        @pl.when(me > 0)
        def _():
            for copy in pair[0]:
                act(copy)

        @pl.when(me < parts - 1)
        def _():
            for copy in pair[1]:
                act(copy)

    def gather(buf, sends, recvs, row):
        return [
            pltpu.make_async_remote_copy(
                buf.at[me], buf.at[me], sends.at[row, k], recvs.at[row, k],
                device_id={"space": (me + k) % parts}, device_id_type=MESH)
            for k in range(1, parts)
        ]

    d = depth
    near = halo(c0, hs, hr, 0, 2, (2 * d - 1, d - 1), (d + 1, 2 * d + 1))
    far = halo(c0, hs, hr, 2, d - 2, (d + 1, 1), (d + 3, 2 * d + 3))
    beyond = halo(c0, hs, hr, 4, 1, (2 * d, 0), (d + 1, 3 * d + 1), reach=2)
    source = halo(src1, hs, hr, 6, 2, (d, 0), (2, d + 2))
    third = halo(c1x, hs, hr, 8, 1, (d, 0), (5, d + 5))
    cap_near = halo(cap, ks, kr, 0, 1, (2 * d - 1, d - 1), (d, 2 * d), rows_at=my_rows)
    cap_far = halo(cap, ks, kr, 2, d - 1, (d, 0), (d + 1, 2 * d + 1), rows_at=my_rows)
    pass_near = hand_on(0, 1, d - 1, 2 * d)
    pass_far = hand_on(2, d - 1, 0, 2 * d + 1)
    gather_cap = gather(gcap, gs, gv, 0)
    gather_r = [gather(gr.at[t], gs, gv, 1 + t) for t in range(steps)]

    def clear(ref, start, stop):
        ref[start:stop] = jnp.zeros((stop - start, rows, lanes), F32)

    @pl.when(me == 0)
    def _():
        clear(cap, 0, d)
        clear(c0, 0, d + 1)
        clear(c1x, 0, 3)
        clear(src1, 0, 2)

    @pl.when(me == 1)
    def _():
        clear(c0, 0, 1)

    @pl.when(me == parts - 2)
    def _():
        clear(c0, 3 * d + 1, 3 * d + 2)

    @pl.when(me == parts - 1)
    def _():
        clear(cap, 2 * d, 3 * d)
        clear(c0, 2 * d + 1, 3 * d + 2)
        clear(c1x, d + 3, d + 6)
        clear(src1, d + 2, d + 4)

    x1p[0] = jnp.zeros(x1p.shape[1:], F32)
    x1p[parts + 1] = jnp.zeros(x1p.shape[1:], F32)

    loads[0].wait()
    mine = cap[d:2 * d]
    gcap[me] = pack(mine)
    loads[1].wait()
    loads[2].wait()
    b = mine * u0[...] + src0[...]
    own[...] = b
    c0[d + 1:2 * d + 1] = b * (W / (mine + 6.0))
    loads[3].wait()

    pl.semaphore_wait(barrier, parts - 1 + spans - 1)
    begin(cap_near)
    begin(near)
    for copy in gather_cap:
        copy.start()

    def weights(start, count):
        plane = (me - 1) * depth + start + iota((count, 1, 1), 0)
        inside = (plane >= 0) & (plane < parts * depth)
        return jnp.where(inside, W / (cap[start:start + count] + 6.0), 0.0)

    arrive(cap_near)
    each(pass_near, lambda copy: copy.start())
    each(pass_near, lambda copy: copy.wait_recv())
    a = weights(d - 1, d + 2)

    for t in range(steps):
        if t == 0:
            arrive(near)
            c = c0[d - 1:2 * d + 3]
        else:
            c = c1x[1:d + 5]
        x = 1.2 * c[1:-1] + a * sum_inner(c, lanes)
        inner = x[1:-1]
        d0 = cap[d:2 * d] + 6.0
        r = own[...] - d0 * inner + sum_inner(x, lanes)
        gr[t, me] = pack(r)
        for copy in gather_r[t]:
            copy.start()
        if t == 1:
            begin(third)
        else:
            begin(cap_far)
            begin(far)
            begin(beyond)
            begin(source)
            for copy in gather_cap:
                copy.wait_recv()
            cap1 = gcap[...]
            i1 = W / (cap1 + 3.0)
            cap2 = to_2(cap1)
            i2 = jnp.where(iota(cap2.shape, 2) < lanes // 4, W / (cap2 + 1.5), 0.0)
            cap3 = to_3(cap2)
            i3 = jnp.where(iota(cap3.shape, 2) < lanes // 8, W / (cap3 + 0.75), 0.0)
            a1, a2, a3 = 0.5 * i1, 0.25 * i2, 0.125 * i3

        for copy in gather_r[t]:
            copy.wait_recv()
        b1 = gr[t]
        c1 = b1 * i1
        y1 = 1.2 * c1 + a1 * sum_packed(c1, half)
        r1 = b1 - (cap1 + 3.0) * y1 + 0.5 * sum_packed(y1, half)
        b2 = to_2(r1)
        c2 = b2 * i2
        y2 = 1.2 * c2 + a2 * sum_planes(c2, lanes // 4)
        r2 = b2 - (cap2 + 1.5) * y2 + 0.25 * sum_planes(y2, lanes // 4)
        c3 = to_3(r2) * i3
        if t == 0:
            arrive(cap_far)
            each(pass_far, lambda copy: copy.start())
        y3 = lax.fori_loop(
            0, COARSE_SWEEPS - 1,
            lambda _, y: (0.2 * y + c3) + a3 * sum_planes(y, lanes // 8), c3, unroll=True)
        lift = twice_rows(dot(flat(y3), up_3), parts // 2)
        lift = jnp.broadcast_to(lift[:, None], (parts // 2, 2) + lift.shape[1:]).reshape(y2.shape)
        y2 = y2 + lift
        for _ in range(2):
            y2 = (0.2 * y2 + c2) + a2 * sum_planes(y2, lanes // 4)
        y1 = y1 + twice_rows(dot(flat(y2), up_2), parts)
        for _ in range(2):
            y1 = (0.2 * y1 + c1) + a1 * sum_packed(y1, half)
        x1p[1:parts + 1] = y1

        n = rows // 2
        around = flat(x1p[pl.ds(me, 3)])
        even, odd = dot(around, up_lo), dot(around, up_hi)
        halves = [part[n * k:n * k + n] for k in range(3) for part in (even, odd)]
        if t == 1:
            halves = halves[1:-1]
        planes = len(halves)
        lift = twice_rows(jnp.concatenate(halves, 0), planes)
        lift = jnp.broadcast_to(lift[:, None], (planes, 2) + lift.shape[1:]).reshape(2 * planes, rows, lanes)
        if t == 0:
            each(pass_far, lambda copy: copy.wait_recv())
            arrive(far)
            arrive(beyond)
            a_lo, a_hi = weights(0, d - 1), weights(2 * d + 1, d - 1)
            first = 1.2 * c0[1:d] + a_lo * sum_inner(c0[0:d + 1], lanes)
            final = 1.2 * c0[2 * d + 2:3 * d + 1] + a_hi * sum_inner(c0[2 * d + 1:3 * d + 2], lanes)
            wide = jnp.concatenate([a_lo, a, a_hi], 0)
            x = jnp.concatenate([first, x, final], 0) + lift
            x = (0.2 * x[1:-1] + c0[2:3 * d]) + wide[1:-1] * sum_inner(x, lanes)
            x = (0.2 * x[1:-1] + c0[3:3 * d - 1]) + wide[2:-2] * sum_inner(x, lanes)
            fp_ref[...] = x[2:-2]
            arrive(source)
            b = cap[2:3 * d - 2] * x + src1[...]
            own[...] = b[2:-2]
            c1x[1:d + 5] = b * wide[2:-2]
        else:
            arrive(third)
            first = 1.2 * c1x[1:2] + wide[2:3] * sum_inner(c1x[0:3], lanes)
            final = 1.2 * c1x[d + 4:d + 5] + wide[-3:-2] * sum_inner(c1x[d + 3:d + 6], lanes)
            x = jnp.concatenate([first, x, final], 0) + lift
            x = (0.2 * x[1:-1] + c1x[2:d + 4]) + a * sum_inner(x, lanes)
            fin[...] = (0.2 * x[1:-1] + c1x[3:d + 3]) + a[1:-1] * sum_inner(x, lanes)

    onward = pltpu.make_async_remote_copy(
        fin, up_ref, ts.at[0], ts.at[1],
        device_id={"tm": (span + 1) % spans}, device_id_type=MESH)

    @pl.when(span < spans - 1)
    def _():
        onward.start()

    @pl.when(span == 0)
    def _():
        up_ref[...] = u0[...]

    for pair in (near, far, beyond, source, third, cap_near, cap_far):
        sent(pair)
    for pair in (pass_near, pass_far):
        each(pair, lambda copy: copy.wait_send())
    for copies in [gather_cap] + gather_r:
        for copy in copies:
            copy.wait_send()

    @pl.when(span < spans - 1)
    def _():
        onward.wait_send()

    @pl.when(span > 0)
    def _():
        onward.wait_recv()


def shards(span_opening, source_power, warmth_retention):
    parts, spans = lax.axis_size("space"), lax.axis_size("tm")
    steps = source_power.shape[1]
    depth, rows, lanes = warmth_retention.shape
    assert steps == 2 and depth == 4
    slab = jax.ShapeDtypeStruct((depth, rows, lanes), F32)
    vmem = pl.BlockSpec(memory_space=pltpu.VMEM)
    dma = pltpu.SemaphoreType.DMA
    fpoint, updated = pl.pallas_call(
        functools.partial(kernel, parts, spans, steps),
        out_shape=(pltpu.VMEM(slab.shape, F32),) * 2,
        in_specs=[pl.BlockSpec(memory_space=pl.ANY)] * 3,
        out_specs=(vmem, vmem),
        scratch_shapes=[
            pltpu.VMEM((depth, rows, lanes), F32),
            pltpu.VMEM((depth, rows, lanes), F32),
            pltpu.VMEM((depth + 4, rows, lanes), F32),
            pltpu.VMEM((3 * depth, rows, lanes), F32),
            pltpu.VMEM((3 * depth + 2, rows, lanes), F32),
            pltpu.VMEM((depth + 6, rows, lanes), F32),
            pltpu.VMEM((parts, rows // 2, lanes), F32),
            pltpu.VMEM((steps, parts, rows // 2, lanes), F32),
            pltpu.VMEM((depth, rows, lanes), F32),
            pltpu.VMEM((parts + 2, rows // 2, lanes), F32),
            pltpu.VMEM((max(parts * rows // 2, 6 * rows), lanes), F32),
            pltpu.VMEM((depth, rows, lanes), F32),
            dma((4,)), dma((10,)), dma((10,)), dma((4,)), dma((4,)), dma((4, spans)), dma((4, spans)),
            dma((1 + steps, parts)), dma((1 + steps, parts)), dma((2,)),
        ],
        compiler_params=pltpu.CompilerParams(
            collective_id=0, has_side_effects=True, vmem_limit_bytes=67043328 - 2 * 4 * slab.size
        ),
    )(span_opening[0], source_power[0], warmth_retention)
    return fpoint[None], updated[None]


def solution(mesh):
    in_specs = (
        P("tm", "space", None, None),
        P("tm", None, "space", None, None),
        P("space", None, None),
    )
    out_specs = (P("tm", "space", None, None), P("tm", "space", None, None))
    return jax.shard_map(shards, mesh=mesh, in_specs=in_specs, out_specs=out_specs, check_vma=False)
```

```python
import functools

import jax
import jax.numpy as jnp
from jax import lax
from jax.experimental import pallas as pl
from jax.experimental.pallas import tpu as pltpu
from jax.sharding import PartitionSpec as P

COARSE_SWEEPS = 24
W = 0.8
F32 = jnp.float32
MESH = pl.DeviceIdType.MESH


def iota(shape, dim):
    return lax.broadcasted_iota(jnp.int32, shape, dim)


def dot(a, b):
    total = None
    for _ in range(3):
        part = a.astype(jnp.bfloat16)
        a = a - part.astype(F32)
        term = jnp.dot(part, b, preferred_element_type=F32)
        total = term if total is None else total + term
    return total


def picks(lanes, pick, scale):
    src, dst = iota((lanes, lanes), 0), iota((lanes, lanes), 1)
    return jnp.where(pick(src, dst), scale, 0.0).astype(jnp.bfloat16)


def in_plane(x, width):
    rows, lanes = x.shape[1], x.shape[2]
    lane, row = iota(x.shape, 2), iota(x.shape, 1)
    left, right = pltpu.roll(x, 1, 2), pltpu.roll(x, lanes - 1, 2)
    if width > lanes // 4:
        left = jnp.where(lane % width == 0, 0.0, left)
        right = jnp.where(lane % width == width - 1, 0.0, right)
    up = jnp.where(row == 0, 0.0, pltpu.roll(x, 1, 1))
    down = jnp.where(row == rows - 1, 0.0, pltpu.roll(x, rows - 1, 1))
    return (left + right) + (up + down)


def shifted(x):
    zero = jnp.zeros((1,) + x.shape[1:], F32)
    return jnp.concatenate([zero, x[:-1]], 0), jnp.concatenate([x[1:], zero], 0)


def sum_planes(x, width):
    before, after = shifted(x)
    return in_plane(x, width) + (before + after)


def sum_packed(x, width):
    half = pltpu.roll(x, width, 2)
    before, after = shifted(half)
    return in_plane(x, width) + (half + jnp.where(iota(x.shape, 2) < width, before, after))


def sum_inner(x, width):
    return in_plane(x[1:-1], width) + (x[:-2] + x[2:])


def column_sum(x):
    rows = x.shape[1]
    row = iota(x.shape, 1)
    before, after = shifted(x)
    up = jnp.where(row == 0, 0.0, pltpu.roll(x, 1, 1))
    down = jnp.where(row == rows - 1, 0.0, pltpu.roll(x, rows - 1, 1))
    return (before + after) + (up + down)


def coarse_solve(c, a, lanes):
    def moved(x):
        return pltpu.roll(x, 1, 2), x, pltpu.roll(x, lanes - 1, 2)

    cs, as_ = moved(c), moved(a)

    def two_sweeps(_, y):
        far = pltpu.roll(y, 2, 2), pltpu.roll(y, lanes - 2, 2)
        near = moved(y)
        sides = far[0] + y, near[0] + near[2], y + far[1]
        once = [
            (0.2 * y_at + c_at) + a_at * (side + column_sum(y_at))
            for y_at, c_at, a_at, side in zip(near, cs, as_, sides)
        ]
        return (0.2 * once[1] + c) + a * ((once[0] + once[2]) + column_sum(once[1]))

    left = COARSE_SWEEPS - 1
    y = c
    if left % 2:
        y = 1.2 * c + a * sum_planes(c, lanes // 8)
    return lax.fori_loop(0, left // 2, two_sweeps, y, unroll=True)


def flat(x):
    return x.reshape(x.shape[0] * x.shape[1], x.shape[2])


def kernel(
    parts, spans, steps,
    open_ref, src_ref, cap_in,
    fp_ref, up_ref,
    u0, src0, src1, cap, c0, c1x, gcap, gr, own, x1p, tmp, fin,
    in_sem, hs, hr, ks, kr, fs, fr, gs, gv, ts,
):
    me, span = lax.axis_index("space"), lax.axis_index("tm")
    depth, rows, lanes = open_ref.shape
    half = lanes // 2

    barrier = pltpu.get_barrier_semaphore()
    for k in range(1, parts):
        pl.semaphore_signal(barrier, inc=1, device_id={"space": (me + k) % parts}, device_id_type=MESH)
    for k in range(1, spans):
        pl.semaphore_signal(barrier, inc=1, device_id={"tm": (span + k) % spans}, device_id_type=MESH)

    loads = [
        pltpu.make_async_copy(cap_in, cap.at[pl.ds(depth, depth)], in_sem.at[0]),
        pltpu.make_async_copy(open_ref, u0, in_sem.at[1]),
        pltpu.make_async_copy(src_ref.at[0], src0, in_sem.at[2]),
        pltpu.make_async_copy(src_ref.at[1], src1.at[pl.ds(2, depth)], in_sem.at[3]),
    ]
    for load in loads:
        load.start()

    down_lo = picks(lanes, lambda s, d: (s // 2 == d) & (d < half), 0.125)
    down_hi = picks(lanes, lambda s, d: s // 2 + half == d, 0.125)
    down_2 = picks(lanes, lambda s, d: (s % half) // 2 == d, 0.125)
    down_3 = picks(lanes, lambda s, d: (s // 2 == d) & (s < half // 2), 0.125)
    up_lo = picks(lanes, lambda s, d: d // 2 == s, 1.0)
    up_hi = picks(lanes, lambda s, d: d // 2 + half == s, 1.0)
    up_2 = picks(lanes, lambda s, d: (d % half) // 2 == s, 1.0)
    up_3 = picks(lanes, lambda s, d: (d // 2 == s) & (d < half // 2), 1.0)

    def pair_rows(x):
        n, r, w = x.shape
        tmp[pl.ds(0, n * r), :] = flat(x)
        return tmp[pl.ds(0, n * r // 2, 2), :] + tmp[pl.ds(1, n * r // 2, 2), :]

    def twice_rows(x, planes):
        r = x.shape[0]
        tmp[pl.ds(0, r, 2), :] = x
        tmp[pl.ds(1, r, 2), :] = x
        return tmp[pl.ds(0, 2 * r), :].reshape(planes, 2 * r // planes, lanes)

    def pack(x):
        s = pair_rows(x.reshape(depth // 2, 2, rows, lanes).sum(1))
        n = rows // 2
        return dot(s[:n], down_lo) + dot(s[n:], down_hi)

    def to_2(x):
        return dot(pair_rows(x), down_2).reshape(parts, rows // 4, lanes)

    def to_3(x):
        s = x.reshape(parts // 2, 2, rows // 4, lanes).sum(1)
        return dot(pair_rows(s), down_3).reshape(parts // 2, rows // 8, lanes)

    def halo(buf, sends, recvs, at, count, up, down, reach=1, rows_at=None):
        def cut(start):
            return buf.at[pl.ds(start, count)] if rows_at is None else buf.at[pl.ds(start, count), rows_at]

        ways = ((up, reach, at), (down, parts - reach, at + 1))
        pair = [
            pltpu.make_async_remote_copy(
                cut(way[0]), cut(way[1]), sends.at[sem], recvs.at[sem],
                device_id={"space": (me + by) % parts}, device_id_type=MESH)
            for way, by, sem in ways
        ]
        return pair + [reach]

    def begin(pair):
        @pl.when(me < parts - pair[2])
        def _():
            pair[0].start()

        @pl.when(me >= pair[2])
        def _():
            pair[1].start()

    def arrive(pair):
        @pl.when(me >= pair[2])
        def _():
            pair[0].wait_recv()

        @pl.when(me < parts - pair[2])
        def _():
            pair[1].wait_recv()

    def sent(pair):
        @pl.when(me < parts - pair[2])
        def _():
            pair[0].wait_send()

        @pl.when(me >= pair[2])
        def _():
            pair[1].wait_send()

    share = rows // spans
    my_rows = pl.ds(pl.multiple_of(span * share, share), share)

    def hand_on(at, count, below, above):
        def copies(start, sem):
            return [
                pltpu.make_async_remote_copy(
                    cap.at[pl.ds(start, count), my_rows], cap.at[pl.ds(start, count), my_rows],
                    fs.at[sem, k], fr.at[sem, k],
                    device_id={"tm": (span + k) % spans}, device_id_type=MESH)
                for k in range(1, spans)
            ]

        return copies(below, at), copies(above, at + 1)

    def each(pair, act):
        @pl.when(me > 0)
        def _():
            for copy in pair[0]:
                act(copy)

        @pl.when(me < parts - 1)
        def _():
            for copy in pair[1]:
                act(copy)

    def gather(buf, sends, recvs, row):
        return [
            pltpu.make_async_remote_copy(
                buf.at[me], buf.at[me], sends.at[row, k], recvs.at[row, k],
                device_id={"space": (me + k) % parts}, device_id_type=MESH)
            for k in range(1, parts)
        ]

    d = depth
    near = halo(c0, hs, hr, 0, 2, (2 * d - 1, d - 1), (d + 1, 2 * d + 1))
    far = halo(c0, hs, hr, 2, d - 2, (d + 1, 1), (d + 3, 2 * d + 3))
    beyond = halo(c0, hs, hr, 4, 1, (2 * d, 0), (d + 1, 3 * d + 1), reach=2)
    source = halo(src1, hs, hr, 6, 2, (d, 0), (2, d + 2))
    third = halo(c1x, hs, hr, 8, 1, (d, 0), (5, d + 5))
    cap_near = halo(cap, ks, kr, 0, 1, (2 * d - 1, d - 1), (d, 2 * d), rows_at=my_rows)
    cap_far = halo(cap, ks, kr, 2, d - 1, (d, 0), (d + 1, 2 * d + 1), rows_at=my_rows)
    pass_near = hand_on(0, 1, d - 1, 2 * d)
    pass_far = hand_on(2, d - 1, 0, 2 * d + 1)
    gather_cap = gather(gcap, gs, gv, 0)
    gather_r = [gather(gr.at[t], gs, gv, 1 + t) for t in range(steps)]

    def clear(ref, start, stop):
        ref[start:stop] = jnp.zeros((stop - start, rows, lanes), F32)

    @pl.when(me == 0)
    def _():
        clear(cap, 0, d)
        clear(c0, 0, d + 1)
        clear(c1x, 0, 3)
        clear(src1, 0, 2)

    @pl.when(me == 1)
    def _():
        clear(c0, 0, 1)

    @pl.when(me == parts - 2)
    def _():
        clear(c0, 3 * d + 1, 3 * d + 2)

    @pl.when(me == parts - 1)
    def _():
        clear(cap, 2 * d, 3 * d)
        clear(c0, 2 * d + 1, 3 * d + 2)
        clear(c1x, d + 3, d + 6)
        clear(src1, d + 2, d + 4)

    x1p[0] = jnp.zeros(x1p.shape[1:], F32)
    x1p[parts + 1] = jnp.zeros(x1p.shape[1:], F32)

    loads[0].wait()
    mine = cap[d:2 * d]
    gcap[me] = pack(mine)
    loads[1].wait()
    loads[2].wait()
    b = mine * u0[...] + src0[...]
    own[...] = b
    c0[d + 1:2 * d + 1] = b * (W / (mine + 6.0))
    loads[3].wait()

    pl.semaphore_wait(barrier, parts - 1 + spans - 1)
    begin(cap_near)
    begin(near)
    for copy in gather_cap:
        copy.start()

    def weights(start, count):
        plane = (me - 1) * depth + start + iota((count, 1, 1), 0)
        inside = (plane >= 0) & (plane < parts * depth)
        return jnp.where(inside, W / (cap[start:start + count] + 6.0), 0.0)

    arrive(cap_near)
    each(pass_near, lambda copy: copy.start())
    each(pass_near, lambda copy: copy.wait_recv())
    a = weights(d - 1, d + 2)

    for t in range(steps):
        if t == 0:
            arrive(near)
            c = c0[d - 1:2 * d + 3]
        else:
            c = c1x[1:d + 5]
        x = 1.2 * c[1:-1] + a * sum_inner(c, lanes)
        inner = x[1:-1]
        d0 = cap[d:2 * d] + 6.0
        r = own[...] - d0 * inner + sum_inner(x, lanes)
        gr[t, me] = pack(r)
        for copy in gather_r[t]:
            copy.start()
        if t == 1:
            begin(third)
        else:
            begin(cap_far)
            begin(far)
            begin(beyond)
            begin(source)
            for copy in gather_cap:
                copy.wait_recv()
            cap1 = gcap[...]
            i1 = W / (cap1 + 3.0)
            cap2 = to_2(cap1)
            i2 = jnp.where(iota(cap2.shape, 2) < lanes // 4, W / (cap2 + 1.5), 0.0)
            cap3 = to_3(cap2)
            i3 = jnp.where(iota(cap3.shape, 2) < lanes // 8, W / (cap3 + 0.75), 0.0)
            a1, a2, a3 = 0.5 * i1, 0.25 * i2, 0.125 * i3

        for copy in gather_r[t]:
            copy.wait_recv()
        b1 = gr[t]
        c1 = b1 * i1
        y1 = 1.2 * c1 + a1 * sum_packed(c1, half)
        r1 = b1 - (cap1 + 3.0) * y1 + 0.5 * sum_packed(y1, half)
        b2 = to_2(r1)
        c2 = b2 * i2
        y2 = 1.2 * c2 + a2 * sum_planes(c2, lanes // 4)
        r2 = b2 - (cap2 + 1.5) * y2 + 0.25 * sum_planes(y2, lanes // 4)
        c3 = to_3(r2) * i3
        if t == 0:
            arrive(cap_far)
            each(pass_far, lambda copy: copy.start())
        y3 = coarse_solve(c3, a3, lanes)
        lift = twice_rows(dot(flat(y3), up_3), parts // 2)
        lift = jnp.broadcast_to(lift[:, None], (parts // 2, 2) + lift.shape[1:]).reshape(y2.shape)
        y2 = y2 + lift
        for _ in range(2):
            y2 = (0.2 * y2 + c2) + a2 * sum_planes(y2, lanes // 4)
        y1 = y1 + twice_rows(dot(flat(y2), up_2), parts)
        for _ in range(2):
            y1 = (0.2 * y1 + c1) + a1 * sum_packed(y1, half)
        x1p[1:parts + 1] = y1

        n = rows // 2
        around = flat(x1p[pl.ds(me, 3)])
        even, odd = dot(around, up_lo), dot(around, up_hi)
        halves = [part[n * k:n * k + n] for k in range(3) for part in (even, odd)]
        if t == 1:
            halves = halves[1:-1]
        planes = len(halves)
        lift = twice_rows(jnp.concatenate(halves, 0), planes)
        lift = jnp.broadcast_to(lift[:, None], (planes, 2) + lift.shape[1:]).reshape(2 * planes, rows, lanes)
        if t == 0:
            each(pass_far, lambda copy: copy.wait_recv())
            arrive(far)
            arrive(beyond)
            a_lo, a_hi = weights(0, d - 1), weights(2 * d + 1, d - 1)
            first = 1.2 * c0[1:d] + a_lo * sum_inner(c0[0:d + 1], lanes)
            final = 1.2 * c0[2 * d + 2:3 * d + 1] + a_hi * sum_inner(c0[2 * d + 1:3 * d + 2], lanes)
            wide = jnp.concatenate([a_lo, a, a_hi], 0)
            x = jnp.concatenate([first, x, final], 0) + lift
            x = (0.2 * x[1:-1] + c0[2:3 * d]) + wide[1:-1] * sum_inner(x, lanes)
            x = (0.2 * x[1:-1] + c0[3:3 * d - 1]) + wide[2:-2] * sum_inner(x, lanes)
            fp_ref[...] = x[2:-2]
            arrive(source)
            b = cap[2:3 * d - 2] * x + src1[...]
            own[...] = b[2:-2]
            c1x[1:d + 5] = b * wide[2:-2]
        else:
            arrive(third)
            first = 1.2 * c1x[1:2] + wide[2:3] * sum_inner(c1x[0:3], lanes)
            final = 1.2 * c1x[d + 4:d + 5] + wide[-3:-2] * sum_inner(c1x[d + 3:d + 6], lanes)
            x = jnp.concatenate([first, x, final], 0) + lift
            x = (0.2 * x[1:-1] + c1x[2:d + 4]) + a * sum_inner(x, lanes)
            fin[...] = (0.2 * x[1:-1] + c1x[3:d + 3]) + a[1:-1] * sum_inner(x, lanes)

    onward = pltpu.make_async_remote_copy(
        fin, up_ref, ts.at[0], ts.at[1],
        device_id={"tm": (span + 1) % spans}, device_id_type=MESH)

    @pl.when(span < spans - 1)
    def _():
        onward.start()

    @pl.when(span == 0)
    def _():
        up_ref[...] = u0[...]

    for pair in (near, far, beyond, source, third, cap_near, cap_far):
        sent(pair)
    for pair in (pass_near, pass_far):
        each(pair, lambda copy: copy.wait_send())
    for copies in [gather_cap] + gather_r:
        for copy in copies:
            copy.wait_send()

    @pl.when(span < spans - 1)
    def _():
        onward.wait_send()

    @pl.when(span > 0)
    def _():
        onward.wait_recv()


def shards(span_opening, source_power, warmth_retention):
    parts, spans = lax.axis_size("space"), lax.axis_size("tm")
    steps = source_power.shape[1]
    depth, rows, lanes = warmth_retention.shape
    assert steps == 2 and depth == 4
    slab = jax.ShapeDtypeStruct((depth, rows, lanes), F32)
    vmem = pl.BlockSpec(memory_space=pltpu.VMEM)
    dma = pltpu.SemaphoreType.DMA
    fpoint, updated = pl.pallas_call(
        functools.partial(kernel, parts, spans, steps),
        out_shape=(pltpu.VMEM(slab.shape, F32),) * 2,
        in_specs=[pl.BlockSpec(memory_space=pl.ANY)] * 3,
        out_specs=(vmem, vmem),
        scratch_shapes=[
            pltpu.VMEM((depth, rows, lanes), F32),
            pltpu.VMEM((depth, rows, lanes), F32),
            pltpu.VMEM((depth + 4, rows, lanes), F32),
            pltpu.VMEM((3 * depth, rows, lanes), F32),
            pltpu.VMEM((3 * depth + 2, rows, lanes), F32),
            pltpu.VMEM((depth + 6, rows, lanes), F32),
            pltpu.VMEM((parts, rows // 2, lanes), F32),
            pltpu.VMEM((steps, parts, rows // 2, lanes), F32),
            pltpu.VMEM((depth, rows, lanes), F32),
            pltpu.VMEM((parts + 2, rows // 2, lanes), F32),
            pltpu.VMEM((max(parts * rows // 2, 6 * rows), lanes), F32),
            pltpu.VMEM((depth, rows, lanes), F32),
            dma((4,)), dma((10,)), dma((10,)), dma((4,)), dma((4,)), dma((4, spans)), dma((4, spans)),
            dma((1 + steps, parts)), dma((1 + steps, parts)), dma((2,)),
        ],
        compiler_params=pltpu.CompilerParams(
            collective_id=0, has_side_effects=True, vmem_limit_bytes=67043328 - 2 * 4 * slab.size
        ),
    )(span_opening[0], source_power[0], warmth_retention)
    return fpoint[None], updated[None]


def solution(mesh):
    in_specs = (
        P("tm", "space", None, None),
        P("tm", None, "space", None, None),
        P("space", None, None),
    )
    out_specs = (P("tm", "space", None, None), P("tm", "space", None, None))
    return jax.shard_map(shards, mesh=mesh, in_specs=in_specs, out_specs=out_specs, check_vma=False)
```

```python
import functools

import jax
import jax.numpy as jnp
from jax import lax
from jax.experimental import pallas as pl
from jax.experimental.pallas import tpu as pltpu
from jax.sharding import PartitionSpec as P

COARSE_SWEEPS = 24
W = 0.8
F32 = jnp.float32
MESH = pl.DeviceIdType.MESH


def iota(shape, dim):
    return lax.broadcasted_iota(jnp.int32, shape, dim)


def dot(a, b):
    total = None
    for _ in range(3):
        part = a.astype(jnp.bfloat16)
        a = a - part.astype(F32)
        term = jnp.dot(part, b, preferred_element_type=F32)
        total = term if total is None else total + term
    return total


def picks(lanes, pick, scale):
    src, dst = iota((lanes, lanes), 0), iota((lanes, lanes), 1)
    return jnp.where(pick(src, dst), scale, 0.0).astype(jnp.bfloat16)


def in_plane(x, width):
    rows, lanes = x.shape[1], x.shape[2]
    lane, row = iota(x.shape, 2), iota(x.shape, 1)
    left, right = pltpu.roll(x, 1, 2), pltpu.roll(x, lanes - 1, 2)
    if width > lanes // 4:
        left = jnp.where(lane % width == 0, 0.0, left)
        right = jnp.where(lane % width == width - 1, 0.0, right)
    up = jnp.where(row == 0, 0.0, pltpu.roll(x, 1, 1))
    down = jnp.where(row == rows - 1, 0.0, pltpu.roll(x, rows - 1, 1))
    return (left + right) + (up + down)


def shifted(x):
    zero = jnp.zeros((1,) + x.shape[1:], F32)
    return jnp.concatenate([zero, x[:-1]], 0), jnp.concatenate([x[1:], zero], 0)


def sum_planes(x, width):
    before, after = shifted(x)
    return in_plane(x, width) + (before + after)


def sum_packed(x, width):
    half = pltpu.roll(x, width, 2)
    before, after = shifted(half)
    return in_plane(x, width) + (half + jnp.where(iota(x.shape, 2) < width, before, after))


def sum_inner(x, width):
    return in_plane(x[1:-1], width) + (x[:-2] + x[2:])


def column_sum(x):
    rows = x.shape[1]
    row = iota(x.shape, 1)
    before, after = shifted(x)
    up = jnp.where(row == 0, 0.0, pltpu.roll(x, 1, 1))
    down = jnp.where(row == rows - 1, 0.0, pltpu.roll(x, rows - 1, 1))
    return (before + after) + (up + down)


def coarse_solve(c, a, lanes):
    def moved(x):
        return pltpu.roll(x, 1, 2), x, pltpu.roll(x, lanes - 1, 2)

    cs, as_ = moved(c), moved(a)

    def two_sweeps(_, y):
        far = pltpu.roll(y, 2, 2), pltpu.roll(y, lanes - 2, 2)
        near = moved(y)
        sides = far[0] + y, near[0] + near[2], y + far[1]
        once = [
            (0.2 * y_at + c_at) + a_at * (side + column_sum(y_at))
            for y_at, c_at, a_at, side in zip(near, cs, as_, sides)
        ]
        return (0.2 * once[1] + c) + a * ((once[0] + once[2]) + column_sum(once[1]))

    left = COARSE_SWEEPS - 1
    y = c
    if left % 2:
        y = 1.2 * c + a * sum_planes(c, lanes // 8)
    return lax.fori_loop(0, left // 2, two_sweeps, y, unroll=True)


def flat(x):
    return x.reshape(x.shape[0] * x.shape[1], x.shape[2])


def kernel(
    parts, spans, steps,
    open_ref, src_ref, cap_in,
    fp_ref, up_ref,
    u0, src0, src1, cap, c0, c1x, gcap, gr, own, x1p, tmp, fin,
    in_sem, hs, hr, ks, kr, fs, fr, gs, gv, ts,
):
    me, span = lax.axis_index("space"), lax.axis_index("tm")
    depth, rows, lanes = open_ref.shape
    half = lanes // 2

    barrier = pltpu.get_barrier_semaphore()
    for k in range(1, parts):
        pl.semaphore_signal(barrier, inc=1, device_id={"space": (me + k) % parts}, device_id_type=MESH)
    for k in range(1, spans):
        pl.semaphore_signal(barrier, inc=1, device_id={"tm": (span + k) % spans}, device_id_type=MESH)

    loads = [
        pltpu.make_async_copy(cap_in, cap.at[pl.ds(depth, depth)], in_sem.at[0]),
        pltpu.make_async_copy(open_ref, u0, in_sem.at[1]),
        pltpu.make_async_copy(src_ref.at[0], src0, in_sem.at[2]),
        pltpu.make_async_copy(src_ref.at[1], src1.at[pl.ds(2, depth)], in_sem.at[3]),
    ]
    for load in loads:
        load.start()

    down_lo = picks(lanes, lambda s, d: (s // 2 == d) & (d < half), 0.125)
    down_hi = picks(lanes, lambda s, d: s // 2 + half == d, 0.125)
    down_2 = picks(lanes, lambda s, d: (s % half) // 2 == d, 0.125)
    down_3 = picks(lanes, lambda s, d: (s // 2 == d) & (s < half // 2), 0.125)
    up_lo = picks(lanes, lambda s, d: d // 2 == s, 1.0)
    up_hi = picks(lanes, lambda s, d: d // 2 + half == s, 1.0)
    up_2 = picks(lanes, lambda s, d: (d % half) // 2 == s, 1.0)
    up_3 = picks(lanes, lambda s, d: (d // 2 == s) & (d < half // 2), 1.0)

    def pair_rows(x):
        n, r, w = x.shape
        tmp[pl.ds(0, n * r), :] = flat(x)
        return tmp[pl.ds(0, n * r // 2, 2), :] + tmp[pl.ds(1, n * r // 2, 2), :]

    def twice_rows(x, planes):
        r = x.shape[0]
        tmp[pl.ds(0, r, 2), :] = x
        tmp[pl.ds(1, r, 2), :] = x
        return tmp[pl.ds(0, 2 * r), :].reshape(planes, 2 * r // planes, lanes)

    def pack(x):
        s = pair_rows(x.reshape(depth // 2, 2, rows, lanes).sum(1))
        n = rows // 2
        return dot(s[:n], down_lo) + dot(s[n:], down_hi)

    def to_2(x):
        return dot(pair_rows(x), down_2).reshape(parts, rows // 4, lanes)

    def to_3(x):
        s = x.reshape(parts // 2, 2, rows // 4, lanes).sum(1)
        return dot(pair_rows(s), down_3).reshape(parts // 2, rows // 8, lanes)

    def halo(buf, sends, recvs, at, count, up, down, reach=1, rows_at=None):
        def cut(start):
            return buf.at[pl.ds(start, count)] if rows_at is None else buf.at[pl.ds(start, count), rows_at]

        ways = ((up, reach, at), (down, parts - reach, at + 1))
        pair = [
            pltpu.make_async_remote_copy(
                cut(way[0]), cut(way[1]), sends.at[sem], recvs.at[sem],
                device_id={"space": (me + by) % parts}, device_id_type=MESH)
            for way, by, sem in ways
        ]
        return pair + [reach]

    def begin(pair):
        @pl.when(me < parts - pair[2])
        def _():
            pair[0].start()

        @pl.when(me >= pair[2])
        def _():
            pair[1].start()

    def arrive(pair):
        @pl.when(me >= pair[2])
        def _():
            pair[0].wait_recv()

        @pl.when(me < parts - pair[2])
        def _():
            pair[1].wait_recv()

    def sent(pair):
        @pl.when(me < parts - pair[2])
        def _():
            pair[0].wait_send()

        @pl.when(me >= pair[2])
        def _():
            pair[1].wait_send()

    share = rows // spans
    my_rows = pl.ds(pl.multiple_of(span * share, share), share)

    def hand_on(at, count, below, above):
        def copies(start, sem):
            return [
                pltpu.make_async_remote_copy(
                    cap.at[pl.ds(start, count), my_rows], cap.at[pl.ds(start, count), my_rows],
                    fs.at[sem, k], fr.at[sem, k],
                    device_id={"tm": (span + k) % spans}, device_id_type=MESH)
                for k in range(1, spans)
            ]

        return copies(below, at), copies(above, at + 1)

    def each(pair, act):
        @pl.when(me > 0)
        def _():
            for copy in pair[0]:
                act(copy)

        @pl.when(me < parts - 1)
        def _():
            for copy in pair[1]:
                act(copy)

    def gather(buf, sends, recvs, row):
        return [
            pltpu.make_async_remote_copy(
                buf.at[me], buf.at[me], sends.at[row, k], recvs.at[row, k],
                device_id={"space": (me + k) % parts}, device_id_type=MESH)
            for k in range(1, parts)
        ]

    d = depth
    near = halo(c0, hs, hr, 0, 2, (2 * d - 1, d - 1), (d + 1, 2 * d + 1))
    far = halo(c0, hs, hr, 2, d - 2, (d + 1, 1), (d + 3, 2 * d + 3))
    beyond = halo(c0, hs, hr, 4, 1, (2 * d, 0), (d + 1, 3 * d + 1), reach=2)
    source = halo(src1, hs, hr, 6, 2, (d, 0), (2, d + 2))
    third = halo(c1x, hs, hr, 8, 1, (d, 0), (5, d + 5))
    cap_near = halo(cap, ks, kr, 0, 1, (2 * d - 1, d - 1), (d, 2 * d), rows_at=my_rows)
    cap_far = halo(cap, ks, kr, 2, d - 1, (d, 0), (d + 1, 2 * d + 1), rows_at=my_rows)
    pass_near = hand_on(0, 1, d - 1, 2 * d)
    pass_far = hand_on(2, d - 1, 0, 2 * d + 1)
    gather_cap = gather(gcap, gs, gv, 0)
    gather_r = [gather(gr.at[t], gs, gv, 1 + t) for t in range(steps)]

    def clear(ref, start, stop):
        ref[start:stop] = jnp.zeros((stop - start, rows, lanes), F32)

    @pl.when(me == 0)
    def _():
        clear(cap, 0, d)
        clear(c0, 0, d + 1)
        clear(c1x, 0, 3)
        clear(src1, 0, 2)

    @pl.when(me == 1)
    def _():
        clear(c0, 0, 1)

    @pl.when(me == parts - 2)
    def _():
        clear(c0, 3 * d + 1, 3 * d + 2)

    @pl.when(me == parts - 1)
    def _():
        clear(cap, 2 * d, 3 * d)
        clear(c0, 2 * d + 1, 3 * d + 2)
        clear(c1x, d + 3, d + 6)
        clear(src1, d + 2, d + 4)

    x1p[0] = jnp.zeros(x1p.shape[1:], F32)
    x1p[parts + 1] = jnp.zeros(x1p.shape[1:], F32)

    loads[0].wait()
    pl.semaphore_wait(barrier, parts - 1 + spans - 1)
    begin(cap_near)
    mine = cap[d:2 * d]
    loads[1].wait()
    loads[2].wait()
    b = mine * u0[...] + src0[...]
    own[...] = b
    c0[d + 1:2 * d + 1] = b * (W / (mine + 6.0))
    begin(near)
    gcap[me] = pack(mine)
    for copy in gather_cap:
        copy.start()
    loads[3].wait()

    def weights(start, count):
        plane = (me - 1) * depth + start + iota((count, 1, 1), 0)
        inside = (plane >= 0) & (plane < parts * depth)
        return jnp.where(inside, W / (cap[start:start + count] + 6.0), 0.0)

    arrive(cap_near)
    each(pass_near, lambda copy: copy.start())
    each(pass_near, lambda copy: copy.wait_recv())
    a = weights(d - 1, d + 2)

    for t in range(steps):
        if t == 0:
            arrive(near)
            c = c0[d - 1:2 * d + 3]
        else:
            c = c1x[1:d + 5]
        x = 1.2 * c[1:-1] + a * sum_inner(c, lanes)
        inner = x[1:-1]
        d0 = cap[d:2 * d] + 6.0
        r = own[...] - d0 * inner + sum_inner(x, lanes)
        gr[t, me] = pack(r)
        for copy in gather_r[t]:
            copy.start()
        if t == 1:
            begin(third)
        else:
            begin(cap_far)
            begin(far)
            begin(beyond)
            begin(source)
            for copy in gather_cap:
                copy.wait_recv()
            cap1 = gcap[...]
            i1 = W / (cap1 + 3.0)
            cap2 = to_2(cap1)
            i2 = jnp.where(iota(cap2.shape, 2) < lanes // 4, W / (cap2 + 1.5), 0.0)
            cap3 = to_3(cap2)
            i3 = jnp.where(iota(cap3.shape, 2) < lanes // 8, W / (cap3 + 0.75), 0.0)
            a1, a2, a3 = 0.5 * i1, 0.25 * i2, 0.125 * i3

        for copy in gather_r[t]:
            copy.wait_recv()
        b1 = gr[t]
        c1 = b1 * i1
        y1 = 1.2 * c1 + a1 * sum_packed(c1, half)
        r1 = b1 - (cap1 + 3.0) * y1 + 0.5 * sum_packed(y1, half)
        b2 = to_2(r1)
        c2 = b2 * i2
        y2 = 1.2 * c2 + a2 * sum_planes(c2, lanes // 4)
        r2 = b2 - (cap2 + 1.5) * y2 + 0.25 * sum_planes(y2, lanes // 4)
        c3 = to_3(r2) * i3
        if t == 0:
            arrive(cap_far)
            each(pass_far, lambda copy: copy.start())
        y3 = coarse_solve(c3, a3, lanes)
        lift = twice_rows(dot(flat(y3), up_3), parts // 2)
        lift = jnp.broadcast_to(lift[:, None], (parts // 2, 2) + lift.shape[1:]).reshape(y2.shape)
        y2 = y2 + lift
        for _ in range(2):
            y2 = (0.2 * y2 + c2) + a2 * sum_planes(y2, lanes // 4)
        y1 = y1 + twice_rows(dot(flat(y2), up_2), parts)
        for _ in range(2):
            y1 = (0.2 * y1 + c1) + a1 * sum_packed(y1, half)
        x1p[1:parts + 1] = y1

        n = rows // 2
        around = flat(x1p[pl.ds(me, 3)])
        even, odd = dot(around, up_lo), dot(around, up_hi)
        halves = [part[n * k:n * k + n] for k in range(3) for part in (even, odd)]
        if t == 1:
            halves = halves[1:-1]
        planes = len(halves)
        lift = twice_rows(jnp.concatenate(halves, 0), planes)
        lift = jnp.broadcast_to(lift[:, None], (planes, 2) + lift.shape[1:]).reshape(2 * planes, rows, lanes)
        if t == 0:
            each(pass_far, lambda copy: copy.wait_recv())
            arrive(far)
            arrive(beyond)
            a_lo, a_hi = weights(0, d - 1), weights(2 * d + 1, d - 1)
            first = 1.2 * c0[1:d] + a_lo * sum_inner(c0[0:d + 1], lanes)
            final = 1.2 * c0[2 * d + 2:3 * d + 1] + a_hi * sum_inner(c0[2 * d + 1:3 * d + 2], lanes)
            wide = jnp.concatenate([a_lo, a, a_hi], 0)
            x = jnp.concatenate([first, x, final], 0) + lift
            x = (0.2 * x[1:-1] + c0[2:3 * d]) + wide[1:-1] * sum_inner(x, lanes)
            x = (0.2 * x[1:-1] + c0[3:3 * d - 1]) + wide[2:-2] * sum_inner(x, lanes)
            fp_ref[...] = x[2:-2]
            arrive(source)
            b = cap[2:3 * d - 2] * x + src1[...]
            own[...] = b[2:-2]
            c1x[1:d + 5] = b * wide[2:-2]
        else:
            arrive(third)
            first = 1.2 * c1x[1:2] + wide[2:3] * sum_inner(c1x[0:3], lanes)
            final = 1.2 * c1x[d + 4:d + 5] + wide[-3:-2] * sum_inner(c1x[d + 3:d + 6], lanes)
            x = jnp.concatenate([first, x, final], 0) + lift
            x = (0.2 * x[1:-1] + c1x[2:d + 4]) + a * sum_inner(x, lanes)
            fin[...] = (0.2 * x[1:-1] + c1x[3:d + 3]) + a[1:-1] * sum_inner(x, lanes)

    onward = pltpu.make_async_remote_copy(
        fin, up_ref, ts.at[0], ts.at[1],
        device_id={"tm": (span + 1) % spans}, device_id_type=MESH)

    @pl.when(span < spans - 1)
    def _():
        onward.start()

    @pl.when(span == 0)
    def _():
        up_ref[...] = u0[...]

    for pair in (near, far, beyond, source, third, cap_near, cap_far):
        sent(pair)
    for pair in (pass_near, pass_far):
        each(pair, lambda copy: copy.wait_send())
    for copies in [gather_cap] + gather_r:
        for copy in copies:
            copy.wait_send()

    @pl.when(span < spans - 1)
    def _():
        onward.wait_send()

    @pl.when(span > 0)
    def _():
        onward.wait_recv()


def shards(span_opening, source_power, warmth_retention):
    parts, spans = lax.axis_size("space"), lax.axis_size("tm")
    steps = source_power.shape[1]
    depth, rows, lanes = warmth_retention.shape
    assert steps == 2 and depth == 4
    slab = jax.ShapeDtypeStruct((depth, rows, lanes), F32)
    vmem = pl.BlockSpec(memory_space=pltpu.VMEM)
    dma = pltpu.SemaphoreType.DMA
    fpoint, updated = pl.pallas_call(
        functools.partial(kernel, parts, spans, steps),
        out_shape=(pltpu.VMEM(slab.shape, F32),) * 2,
        in_specs=[pl.BlockSpec(memory_space=pl.ANY)] * 3,
        out_specs=(vmem, vmem),
        scratch_shapes=[
            pltpu.VMEM((depth, rows, lanes), F32),
            pltpu.VMEM((depth, rows, lanes), F32),
            pltpu.VMEM((depth + 4, rows, lanes), F32),
            pltpu.VMEM((3 * depth, rows, lanes), F32),
            pltpu.VMEM((3 * depth + 2, rows, lanes), F32),
            pltpu.VMEM((depth + 6, rows, lanes), F32),
            pltpu.VMEM((parts, rows // 2, lanes), F32),
            pltpu.VMEM((steps, parts, rows // 2, lanes), F32),
            pltpu.VMEM((depth, rows, lanes), F32),
            pltpu.VMEM((parts + 2, rows // 2, lanes), F32),
            pltpu.VMEM((max(parts * rows // 2, 6 * rows), lanes), F32),
            pltpu.VMEM((depth, rows, lanes), F32),
            dma((4,)), dma((10,)), dma((10,)), dma((4,)), dma((4,)), dma((4, spans)), dma((4, spans)),
            dma((1 + steps, parts)), dma((1 + steps, parts)), dma((2,)),
        ],
        compiler_params=pltpu.CompilerParams(
            collective_id=0, has_side_effects=True, vmem_limit_bytes=67043328 - 2 * 4 * slab.size
        ),
    )(span_opening[0], source_power[0], warmth_retention)
    return fpoint[None], updated[None]


def solution(mesh):
    in_specs = (
        P("tm", "space", None, None),
        P("tm", None, "space", None, None),
        P("space", None, None),
    )
    out_specs = (P("tm", "space", None, None), P("tm", "space", None, None))
    return jax.shard_map(shards, mesh=mesh, in_specs=in_specs, out_specs=out_specs, check_vma=False)
```
